32 devices in a mesh: dp: 2 (over z, core), sp: 16 (over x, y).
Axes of the slice: x: 4, y: 4, z: 1, core: 2. Of those that a mesh axis runs over, the one named last changes fastest.
The devices are a block of a 4x4x8 slice.
Arguments:
- x: bfloat16 [8192, 4096], P(('dp', 'sp')), parts along dimension 0
- gain: bfloat16 [4096], replicated
- wq: bfloat16 [4096, 4096], replicated
- wk: bfloat16 [4096, 4096], replicated
- wv: bfloat16 [4096, 4096], replicated
- wo: bfloat16 [4096, 4096], replicated
Outputs:
- output: bfloat16 [8192, 4096], P(('dp', 'sp')), parts along dimension 0
There are 2 independent parts. The reference program is written for one: setup_inputs(seed, part) draws one part's arguments, and reference() takes and returns one part's arrays. A program takes and returns all parts, laid end to end along the dimension named above; an argument that names none is the same for every part.
All inputs are finite; a program needn't handle non-finite values.
Results may differ from the reference program's by a relative error of at most 0.012.
Values are sent between devices in bfloat16 or wider.
A program may use at most 768 MiB of HBM per device.

```python
import jax
import jax.numpy as jnp
from jax import lax

ROWS = 4096
D = 4096
HEADS = 16
KV_HEADS = 16
HEAD = 256
THETA = 10000


def setup_inputs(seed: int = 0, part: int = 0) -> dict:
    kx, kn, kq, kk, kv, ko = jax.random.split(jax.random.key(seed), 6)

    def weights(key, rows, columns):
        return jax.random.normal(key, (rows, columns), jnp.float32) * rows**-0.5

    drawn = {
        "x": jax.random.normal(jax.random.fold_in(kx, part), (ROWS, D), jnp.float32),
        "gain": 1 + 0.1 * jax.random.normal(kn, (D,), jnp.float32),
        "wq": 2 * weights(kq, D, HEADS * HEAD),
        "wk": 2 * weights(kk, D, KV_HEADS * HEAD),
        "wv": 4 * weights(kv, D, KV_HEADS * HEAD),
        "wo": weights(ko, HEADS * HEAD, D),
    }
    return {k: v.astype(jnp.bfloat16) for k, v in drawn.items()}


def normed(x, gain):
    wide = x.astype(jnp.float32)
    scale = lax.rsqrt(jnp.mean(wide * wide, -1, keepdims=True) + 1e-6)
    return (wide * scale * gain.astype(jnp.float32)).astype(jnp.bfloat16)


def turned(t, place, theta):
    half = t.shape[-1] // 2
    angle = place.astype(jnp.float32)[:, None] * theta ** (-jnp.arange(half, dtype=jnp.float32) / half)
    cos, sin = jnp.cos(angle)[:, None], jnp.sin(angle)[:, None]
    a, b = t[..., :half].astype(jnp.float32), t[..., half:].astype(jnp.float32)
    return jnp.concatenate([a * cos - b * sin, b * cos + a * sin], -1).astype(jnp.bfloat16)


def matmul(a, w):
    return jnp.dot(a, w, preferred_element_type=jnp.float32).astype(jnp.bfloat16)


def einsum(form, a, b):
    return jnp.einsum(form, a.astype(jnp.float32), b.astype(jnp.float32))


def attention(q, k, v):
    scores = einsum("tgsd,ugd->gstu", q, k) * q.shape[-1] ** -0.5
    token = jnp.arange(q.shape[0])
    scores = jnp.where(token[:, None] >= token, scores, -jnp.inf)
    weights = jax.nn.softmax(scores, -1).astype(jnp.bfloat16)
    return einsum("gstu,ugd->tgsd", weights, v).astype(jnp.bfloat16)


def reference(x, gain, wq, wk, wv, wo):
    a, place = normed(x, gain), jnp.arange(ROWS)
    q = turned(matmul(a, wq).reshape(ROWS, HEADS, HEAD), place, THETA).reshape(ROWS, KV_HEADS, -1, HEAD)
    k = turned(matmul(a, wk).reshape(ROWS, KV_HEADS, HEAD), place, THETA)
    v = matmul(a, wv).reshape(ROWS, KV_HEADS, HEAD)
    seen = attention(q, k, v).reshape(ROWS, HEADS * HEAD)
    return (x.astype(jnp.float32) + jnp.dot(seen, wo, preferred_element_type=jnp.float32)).astype(jnp.bfloat16)
```

```python
import functools
import math

import jax
import jax.numpy as jnp
from jax import lax
from jax.experimental import pallas as pl
from jax.experimental.pallas import tpu as pltpu
from jax.sharding import PartitionSpec as P

HEAD = 256
THETA = 10000
NEG = -1e30
HIDDEN = 2 * NEG
LOG2E = 1.4426950408889634
MESH = pl.DeviceIdType.MESH
SLOTS = 3


def _dot(a, b, ca=1, cb=0):
    return lax.dot_general(a, b, (((ca,), (cb,)), ((), ())), preferred_element_type=jnp.float32)


def _order(n):
    side = math.isqrt(n)
    if side * side != n:
        return n, [(0, i) for i in range(1, n)] + [(0, 0)]
    far = lambda d: min(d, side - d)
    offsets = [(a, b) for a in range(side) for b in range(side)]
    turn = lambda o: (far(o[0]) + far(o[1]), max(far(o[0]), far(o[1])), min(o[0], o[1]) > 0 and o[0] != o[1], o[0] == 0)
    offsets.sort(key=turn)
    return side, offsets[1:] + offsets[:1]


def _pick(t, values):
    out = jnp.int32(values[-1])
    for i, v in enumerate(values[:-1]):
        out = jnp.where(t == i, jnp.int32(v), out)
    return out


def _places(n, me):
    side, offsets = _order(n)
    high, low = me // side, lax.rem(me, side)
    rows = n // side

    def to(t):
        a, b = _pick(t, [o[0] for o in offsets]), _pick(t, [o[1] for o in offsets])
        return lax.rem(high + a, rows) * side + lax.rem(low + b, side)

    def frm(t):
        a, b = _pick(t, [o[0] for o in offsets]), _pick(t, [o[1] for o in offsets])
        return lax.rem(high - a + rows, rows) * side + lax.rem(low - b + side, side)

    return to, frm


def _greet(n, me):
    barrier = pltpu.get_barrier_semaphore()

    def tell(i, _):
        pl.semaphore_signal(barrier, inc=1, device_id={"sp": lax.rem(me + i, n)}, device_id_type=MESH)

    lax.fori_loop(1, n, tell, None)
    return lambda: pl.semaphore_wait(barrier, n - 1)


def _project(n, x_ref, gain_ref, cos_ref, sin_ref, wq_ref, wk_ref, wv_ref, q_ref, k_ref, v_ref, a_s, w_s, out_s, w_sem, send_sem, recv_sem,
             own_sem):
    me = lax.axis_index("sp")
    to, frm = _places(n, me)
    everyone = _greet(n, me)
    own = x_ref.shape[0]
    work = ((wk_ref, k_ref), (wv_ref, v_ref), (wq_ref, q_ref))

    def fetch(m, t):
        slot = lax.rem(m * n + t, SLOTS)
        return pltpu.make_async_copy(work[m][0].at[:, pl.ds(pl.multiple_of(to(t) * HEAD, HEAD), HEAD)], w_s.at[slot], w_sem.at[slot])

    for t in range(SLOTS - 1):
        fetch(0, t).start()

    rows = 32

    def norm(i, _):
        here = pl.ds(pl.multiple_of(i * rows, rows), rows)
        wide = x_ref[here, :].astype(jnp.float32)
        scale = lax.rsqrt(jnp.mean(wide * wide, -1, keepdims=True) + 1e-6)
        a_s[here, :] = (wide * scale * gain_ref[...].astype(jnp.float32)).astype(jnp.bfloat16)

    lax.fori_loop(0, own // rows, norm, None)
    everyone()

    def send(m, t, block, device):
        i = m * n + t
        return pltpu.make_async_remote_copy(out_s.at[i], work[m][1].at[block], send_sem.at[i], recv_sem.at[i], device_id={"sp": device},
                                            device_id_type=MESH)

    def keep(m):
        return pltpu.make_async_copy(out_s.at[m * n + n - 1], work[m][1].at[me], own_sem.at[m])

    for m in range(3):

        def step(t, _, m=m):
            ahead = t + SLOTS - 1

            @pl.when(ahead < n)
            def _():
                fetch(m, ahead).start()

            if m < 2:
                @pl.when(ahead >= n)
                def _():
                    fetch(m + 1, ahead - n).start()

            @pl.when(t > 0)
            def _():
                send(m, t - 1, me, to(t - 1)).start()

            fetch(m, t).wait()
            made = _dot(a_s[...], w_s[lax.rem(m * n + t, SLOTS)]).astype(jnp.bfloat16)
            if m == 1:
                out_s[m * n + t] = made.astype(jnp.float32).T.astype(jnp.bfloat16)
            else:
                a, b = made[:, : HEAD // 2].astype(jnp.float32), made[:, HEAD // 2 :].astype(jnp.float32)
                cos, sin = cos_ref[...], sin_ref[...]
                out_s[m * n + t, :, : HEAD // 2] = (a * cos - b * sin).astype(jnp.bfloat16)
                out_s[m * n + t, :, HEAD // 2 :] = (b * cos + a * sin).astype(jnp.bfloat16)

        lax.fori_loop(0, n, step, None)
        keep(m).start()

    for m in range(3):
        keep(m).wait()

        def done(t, _, m=m):
            send(m, t, me, to(t)).wait_send()
            send(m, t, frm(t), to(t)).wait_recv()

        lax.fori_loop(0, n - 1, done, None)


def _attend(n, q_ref, k_ref, v_ref, x_ref, wo_ref, y_ref, q_s, k_s, v_s, wo_s, o_s, seen_s, top_s, mix_s, in_sem, wo_sem, send_sem, recv_sem,
            own_sem):
    me = lax.axis_index("sp")
    everyone = _greet(n, me)
    own = q_s.shape[1]
    loads = [pltpu.make_async_copy(a, b, in_sem.at[i]) for i, (a, b) in enumerate(((k_ref, k_s), (q_ref, q_s), (v_ref, v_s)))]
    for load in loads:
        load.start()
    width = wo_s.shape[2]

    def fetch(i):
        return pltpu.make_async_copy(wo_ref.at[:, pl.ds(pl.multiple_of(i * width, width), width)], wo_s.at[i], wo_sem.at[i])

    for i in range(wo_s.shape[0]):
        fetch(i).start()
    for load in loads:
        load.wait()
    everyone()

    e = HEAD**-0.5 * LOG2E
    two = 2
    size = two * own
    ones = jnp.ones((8, size), jnp.bfloat16)

    def block(p, j, masked):
        keys = k_s[pl.ds(j * two, two)].reshape(size, HEAD)
        values = jnp.concatenate([jnp.concatenate([v_s[j * two + i] for i in range(two)], axis=1), ones], axis=0)
        scores = [_dot(keys, q_s[p * two + i], 1, 1) for i in range(two)]
        weights, keeps = [], []
        for i, s in enumerate(scores):
            if masked:
                gap = lax.broadcasted_iota(jnp.int32, s.shape, 1) - lax.broadcasted_iota(jnp.int32, s.shape, 0)
                s = jnp.where(gap >= -i * own, s, HIDDEN)
            old = top_s[i : i + 1, :]
            top = jnp.maximum(old, s.max(axis=0, keepdims=True))
            top_s[i : i + 1, :] = top
            weights.append(jnp.exp2((s - top) * e).astype(jnp.bfloat16))
            keeps.append(jnp.exp2((old - top) * e))
        for i in range(two):
            mix_s[i] = mix_s[i] * keeps[i] + _dot(values, weights[i])

    def copy(dest, head):
        return pltpu.make_async_remote_copy(o_s.at[dest], seen_s.at[:, pl.ds(pl.multiple_of(head * HEAD, HEAD), HEAD)], send_sem.at[dest],
                                            recv_sem.at[head], device_id={"sp": dest}, device_id_type=MESH)

    def keep():
        return pltpu.make_async_copy(o_s.at[me], seen_s.at[:, pl.ds(pl.multiple_of(me * HEAD, HEAD), HEAD)], own_sem)

    blocks = n // two

    def run(i, _):
        u = lax.rem(me + i // 2, blocks // 2)
        p = jnp.where(lax.rem(i, 2) == 0, u, blocks - 1 - u)
        top_s[...] = jnp.full_like(top_s, NEG)
        mix_s[...] = jnp.zeros_like(mix_s)
        lax.fori_loop(0, p, lambda j, _: block(p, j, False), None)
        block(p, p, True)
        for i in range(two):
            total = mix_s[i, HEAD : HEAD + 1, :]
            o_s[p * two + i] = (mix_s[i, :HEAD, :] * (1 / total)).T.astype(jnp.bfloat16)
        for i in range(two):
            dest = p * two + i

            @pl.when(dest != me)
            def _():
                copy(dest, me).start()

            @pl.when(dest == me)
            def _():
                keep().start()

    lax.fori_loop(0, blocks, run, None)
    keep().wait()

    def done(i, _):
        other = lax.rem(me + i, n)
        copy(other, me).wait_send()
        copy(other, other).wait_recv()

    lax.fori_loop(1, n, done, None)

    def out(i, _):
        fetch(i).wait()
        here = pl.ds(pl.multiple_of(i * width, width), width)
        y_ref[:, here] = (x_ref[:, here].astype(jnp.float32) + _dot(seen_s[...], wo_s[i])).astype(jnp.bfloat16)

    lax.fori_loop(0, wo_s.shape[0], out, None)


def solution(mesh):
    n = mesh.shape["sp"]
    any_, vmem = pl.BlockSpec(memory_space=pl.ANY), pl.BlockSpec(memory_space=pltpu.VMEM)
    low = jnp.bfloat16

    def step(x, gain, wq, wk, wv, wo):
        own, d = x.shape
        half = HEAD // 2
        place = (lax.axis_index("sp") * own + jnp.arange(own)).astype(jnp.float32)
        angle = place[:, None] * THETA ** (-jnp.arange(half, dtype=jnp.float32) / half)
        blocks = jax.ShapeDtypeStruct((n, own, HEAD), low)
        q, k, v = pl.pallas_call(
            functools.partial(_project, n),
            out_shape=[blocks] * 3,
            in_specs=[vmem] * 4 + [any_] * 3,
            out_specs=[any_] * 3,
            scratch_shapes=[
                pltpu.VMEM((own, d), low),
                pltpu.VMEM((SLOTS, d, HEAD), low),
                pltpu.VMEM((3 * n, own, HEAD), low),
                pltpu.SemaphoreType.DMA((SLOTS,)),
                pltpu.SemaphoreType.DMA((3 * n,)),
                pltpu.SemaphoreType.DMA((3 * n,)),
                pltpu.SemaphoreType.DMA((3,)),
            ],
            compiler_params=pltpu.CompilerParams(collective_id=0, has_side_effects=True, vmem_limit_bytes=48 * 2**20),
            cost_estimate=pl.CostEstimate(flops=6 * own * d * d, transcendentals=0, bytes_accessed=6 * d * d),
        )(x, gain[None], jnp.cos(angle), jnp.sin(angle), wq, wk, wv)
        width = 512
        return pl.pallas_call(
            functools.partial(_attend, n),
            out_shape=jax.ShapeDtypeStruct((own, d), low),
            in_specs=[any_] * 3 + [vmem, any_],
            out_specs=vmem,
            scratch_shapes=[
                pltpu.VMEM((n, own, HEAD), low),
                pltpu.VMEM((n, own, HEAD), low),
                pltpu.VMEM((n, HEAD, own), low),
                pltpu.VMEM((d // width, wo.shape[0], width), low),
                pltpu.VMEM((n, own, HEAD), low),
                pltpu.VMEM((own, n * HEAD), low),
                pltpu.VMEM((2, own), jnp.float32),
                pltpu.VMEM((2, HEAD + 8, own), jnp.float32),
                pltpu.SemaphoreType.DMA((3,)),
                pltpu.SemaphoreType.DMA((d // width,)),
                pltpu.SemaphoreType.DMA((n,)),
                pltpu.SemaphoreType.DMA((n,)),
                pltpu.SemaphoreType.DMA,
            ],
            compiler_params=pltpu.CompilerParams(collective_id=1, has_side_effects=True, vmem_limit_bytes=60 * 2**20),
            cost_estimate=pl.CostEstimate(flops=4 * own * d * d, transcendentals=0, bytes_accessed=2 * d * d),
        )(q, k, v, x, wo)

    tokens, whole = P(("dp", "sp"), None), P(None, None)
    return jax.shard_map(
        step,
        mesh=mesh,
        in_specs=(tokens, P(None), whole, whole, whole, whole),
        out_specs=tokens,
        check_vma=False,
    )
```

```python
import functools
import math

import jax
import jax.numpy as jnp
from jax import lax
from jax.experimental import pallas as pl
from jax.experimental.pallas import tpu as pltpu
from jax.sharding import PartitionSpec as P

HEAD = 256
THETA = 10000
NEG = -1e30
HIDDEN = 2 * NEG
LOG2E = 1.4426950408889634
MESH = pl.DeviceIdType.MESH
SLOTS = 3
TWO = 2
WIDTH = 512


def _dot(a, b, ca=1, cb=0):
    return lax.dot_general(a, b, (((ca,), (cb,)), ((), ())), preferred_element_type=jnp.float32)


def _offsets(side):
    far = lambda d: min(d, side - d)
    offsets = [(a, b) for a in range(side) for b in range(side)]
    offsets.sort(key=lambda o: (far(o[0]) + far(o[1]), max(far(o[0]), far(o[1])), min(o[0], o[1]) > 0 and o[0] != o[1], o[0] == 0))
    return offsets[1:] + offsets[:1]


def _pick(t, values):
    out = jnp.int32(values[-1])
    for i, v in enumerate(values[:-1]):
        out = jnp.where(t == i, jnp.int32(v), out)
    return out


def _flip(u, t):
    return lax.rem(u + t, 2) + 2 * lax.rem(u // 2 + t // 2, 2)


def _kernel(n, x_ref, gain_ref, cos_ref, sin_ref, wq_ref, wk_ref, wv_ref, wo_ref, y_ref, x_s, a_s, w_s, out_s, q_s, k_s, v_s, wo_s, seen_s, acc_s,
            top_s, mix_s, x_sem, w_sem, wo_sem, send_sem, recv_sem, own_sem, back_send, back_recv, back_own, y_sem):
    side = math.isqrt(n)
    me = lax.axis_index("sp")
    high, low = me // side, lax.rem(me, side)
    own = x_s.shape[0]
    blocks = n // TWO
    offsets = _offsets(side)

    def to(t):
        a, b = _pick(t, [o[0] for o in offsets]), _pick(t, [o[1] for o in offsets])
        return lax.rem(high + a, side) * side + lax.rem(low + b, side)

    def frm(t):
        a, b = _pick(t, [o[0] for o in offsets]), _pick(t, [o[1] for o in offsets])
        return lax.rem(high - a + side, side) * side + lax.rem(low - b + side, side)

    def pair(r):
        return _flip(lax.rem(low + 2 * high, side), r)

    def attends(i):
        r, a = i // side, lax.rem(i, side)
        p = me // TWO
        u = _flip(jnp.minimum(p, blocks - 1 - p), r)
        return a * side + lax.rem(u + 2 * a, side)

    serves = (to, to, attends)
    work = ((wk_ref, k_s), (wv_ref, v_s), (wq_ref, q_s))

    barrier = pltpu.get_barrier_semaphore()

    def greet(i, _):
        pl.semaphore_signal(barrier, inc=1, device_id={"sp": lax.rem(me + i, n)}, device_id_type=MESH)

    lax.fori_loop(1, n, greet, None)

    def fetch(m, t):
        slot = lax.rem(m * n + t, SLOTS)
        columns = pl.ds(pl.multiple_of(serves[m](t) * HEAD, HEAD), HEAD)
        return pltpu.make_async_copy(work[m][0].at[:, columns], w_s.at[slot], w_sem.at[slot])

    get_x = pltpu.make_async_copy(x_ref, x_s, x_sem)
    get_x.start()
    for t in range(SLOTS - 1):
        fetch(0, t).start()
    get_x.wait()

    rows = 32

    def norm(i, _):
        here = pl.ds(pl.multiple_of(i * rows, rows), rows)
        wide = x_s[here, :].astype(jnp.float32)
        scale = lax.rsqrt(jnp.mean(wide * wide, -1, keepdims=True) + 1e-6)
        a_s[here, :] = (wide * scale * gain_ref[...].astype(jnp.float32)).astype(jnp.bfloat16)

    lax.fori_loop(0, own // rows, norm, None)
    pl.semaphore_wait(barrier, n - 1)

    def send(m, t, place, device):
        return pltpu.make_async_remote_copy(out_s.at[m * n + t], work[m][1].at[place], send_sem.at[m * n + t], recv_sem.at[m * n + place],
                                            device_id={"sp": device}, device_id_type=MESH)

    def keep(m, t):
        return pltpu.make_async_copy(out_s.at[m * n + t], work[m][1].at[me], own_sem.at[m])

    def pass_on(m, t):
        device = serves[m](t)

        @pl.when(device != me)
        def _():
            send(m, t, me, device).start()

        @pl.when(device == me)
        def _():
            keep(m, t).start()

    for m in range(3):

        def step(t, _, m=m):
            ahead = t + SLOTS - 1

            @pl.when(ahead < n)
            def _():
                fetch(m, ahead).start()

            if m < 2:
                @pl.when(ahead >= n)
                def _():
                    fetch(m + 1, ahead - n).start()

            @pl.when(t > 0)
            def _():
                pass_on(m, t - 1)

            fetch(m, t).wait()
            made = _dot(a_s[...], w_s[lax.rem(m * n + t, SLOTS)]).astype(jnp.bfloat16).astype(jnp.float32)
            if m != 1:
                a, b = made[:, : HEAD // 2], made[:, HEAD // 2 :]
                cos, sin = cos_ref[...], sin_ref[...]
                made = jnp.concatenate([a * cos - b * sin, b * cos + a * sin], axis=1)
            if m != 0:
                made = made.T
            out_s[m * n + t] = made.astype(jnp.bfloat16)

        lax.fori_loop(0, n, step, None)
        pass_on(m, n - 1)

    def fetch_out(i):
        return pltpu.make_async_copy(wo_ref.at[pl.ds(pl.multiple_of(attends(i) * HEAD, HEAD), HEAD), :], wo_s.at[i], wo_sem.at[i])

    lax.fori_loop(0, n, lambda i, _: fetch_out(i).start(), None)
    acc_s[...] = x_s[...].astype(jnp.float32)

    for m in range(2):
        keep(m, n - 1).wait()

        def came(t, _, m=m):
            send(m, t, me, to(t)).wait_send()
            send(m, t, frm(t), to(t)).wait_recv()

        lax.fori_loop(0, n - 1, came, None)
    keep(2, 0).wait()

    e = HEAD**-0.5 * LOG2E
    size = TWO * own

    def block(p, j, many, masked):
        keys = [k_s[pl.ds((j + c) * TWO, TWO)].reshape(size, HEAD) for c in range(many)]
        values = jnp.concatenate([v_s[j * TWO + c] for c in range(TWO * many)], axis=1)
        values = jnp.concatenate([values, jnp.ones((8, size * many), jnp.bfloat16)], axis=0)
        scores = [[_dot(some, q_s[p * TWO + i]) for some in keys] for i in range(TWO)]
        weights, keeps = [], []
        for i, parts in enumerate(scores):
            if masked:
                gap = lax.broadcasted_iota(jnp.int32, (size, own), 1) - lax.broadcasted_iota(jnp.int32, (size, own), 0)
                parts[-1] = jnp.where(gap >= -i * own, parts[-1], HIDDEN)
            old = top_s[i : i + 1, :]
            top = old
            for s in parts:
                top = jnp.maximum(top, s.max(axis=0, keepdims=True))
            top_s[i : i + 1, :] = top
            weights.append(jnp.concatenate([jnp.exp2((s - top) * e).astype(jnp.bfloat16) for s in parts], axis=0))
            keeps.append(jnp.exp2((old - top) * e))
        for i in range(TWO):
            mix_s[i] = mix_s[i] * keeps[i] + _dot(values, weights[i])

    def seen(r, a):
        return seen_s.at[r, :, pl.ds(pl.multiple_of(a * HEAD, HEAD), HEAD)]

    def back(dest, r, a):
        return pltpu.make_async_remote_copy(out_s.at[dest], seen(r, a), back_send.at[dest], back_recv.at[r * side + a], device_id={"sp": dest},
                                            device_id_type=MESH)

    def back_keep(r):
        return pltpu.make_async_copy(out_s.at[me], seen(r, high), back_own)

    def attend(i, _):
        r = i // 2
        u = pair(r)
        p = jnp.where(lax.rem(i, 2) == 0, u, blocks - 1 - u)
        for c in range(TWO):
            source = p * TWO + c

            @pl.when(source != me)
            def _():
                send(2, 0, source, source).wait_recv()

        top_s[...] = jnp.full_like(top_s, NEG)
        mix_s[...] = jnp.zeros_like(mix_s)
        lax.fori_loop(0, p // 2, lambda j, _: block(p, 2 * j, 2, False), None)

        @pl.when(lax.rem(p, 2) == 1)
        def _():
            block(p, p - 1, 2, True)

        @pl.when(lax.rem(p, 2) == 0)
        def _():
            block(p, p, 1, True)

        for c in range(TWO):
            total = mix_s[c, HEAD : HEAD + 1, :]
            out_s[p * TWO + c] = (mix_s[c, :HEAD, :] * (1 / total)).T.astype(jnp.bfloat16)
        for c in range(TWO):
            dest = p * TWO + c

            @pl.when(dest != me)
            def _():
                back(dest, r, high).start()

            @pl.when(dest == me)
            def _():
                back_keep(r).start()

    lax.fori_loop(0, blocks, attend, None)

    def left(t, _):
        device = attends(t)

        @pl.when(device != me)
        def _():
            send(2, t, me, device).wait_send()

    def arrive(r):
        for a in range(side):
            head = attends(r * side + a)

            @pl.when(head != me)
            def _():
                back(head, r, a).wait_recv()

            @pl.when(head == me)
            def _():
                back_keep(r).wait()

            fetch_out(r * side + a).wait()

    def weights_of(r, here):
        return wo_s[pl.ds(r * side, side), :, here].reshape(side * HEAD, WIDTH)

    def columns(c):
        return pl.ds(pl.multiple_of(c * WIDTH, WIDTH), WIDTH)

    def gather(r, _):
        arrive(r)

        def part(c, _):
            here = columns(c)
            acc_s[:, here] += _dot(seen_s[r], weights_of(r, here))

        lax.fori_loop(0, acc_s.shape[1] // WIDTH, part, None)

    lax.fori_loop(0, side - 1, gather, None)
    arrive(side - 1)

    def put(c):
        return pltpu.make_async_copy(x_s.at[:, columns(c)], y_ref.at[:, columns(c)], y_sem.at[c])

    def last(c, _):
        here = columns(c)
        x_s[:, here] = (acc_s[:, here] + _dot(seen_s[side - 1], weights_of(side - 1, here))).astype(jnp.bfloat16)
        put(c).start()

    chunks = acc_s.shape[1] // WIDTH
    lax.fori_loop(0, chunks, last, None)
    lax.fori_loop(0, n, left, None)

    def gone(i, _):
        dest = lax.rem(me + i, n)
        back(dest, 0, 0).wait_send()

    lax.fori_loop(1, n, gone, None)
    lax.fori_loop(0, chunks, lambda c, _: put(c).wait(), None)


def solution(mesh):
    n = mesh.shape["sp"]
    side = math.isqrt(n)
    any_, vmem = pl.BlockSpec(memory_space=pl.ANY), pl.BlockSpec(memory_space=pltpu.VMEM)
    low, wide = jnp.bfloat16, jnp.float32

    def step(x, gain, wq, wk, wv, wo):
        own, d = x.shape
        half = HEAD // 2
        place = (lax.axis_index("sp") * own + jnp.arange(own)).astype(wide)
        angle = place[:, None] * THETA ** (-jnp.arange(half, dtype=wide) / half)
        dma = lambda *shape: pltpu.SemaphoreType.DMA(shape)
        return pl.pallas_call(
            functools.partial(_kernel, n),
            out_shape=jax.ShapeDtypeStruct((own, d), low),
            in_specs=[any_] + [vmem] * 3 + [any_] * 4,
            out_specs=any_,
            scratch_shapes=[
                pltpu.VMEM((own, d), low),
                pltpu.VMEM((own, d), low),
                pltpu.VMEM((SLOTS, d, HEAD), low),
                pltpu.VMEM((3 * n, own, HEAD), low),
                pltpu.VMEM((n, HEAD, own), low),
                pltpu.VMEM((n, own, HEAD), low),
                pltpu.VMEM((n, HEAD, own), low),
                pltpu.VMEM((n, HEAD, d), low),
                pltpu.VMEM((side, own, side * HEAD), low),
                pltpu.VMEM((own, d), wide),
                pltpu.VMEM((TWO, own), wide),
                pltpu.VMEM((TWO, HEAD + 8, own), wide),
                dma(), dma(SLOTS), dma(n), dma(3 * n), dma(3 * n), dma(3), dma(n), dma(n), dma(), dma(d // WIDTH),
            ],
            compiler_params=pltpu.CompilerParams(collective_id=0, has_side_effects=True, vmem_limit_bytes=67043328),
            cost_estimate=pl.CostEstimate(flops=10 * own * d * d, transcendentals=0, bytes_accessed=8 * d * d),
        )(x, gain[None], jnp.cos(angle), jnp.sin(angle), wq, wk, wv, wo)

    tokens, whole = P(("dp", "sp"), None), P(None, None)
    return jax.shard_map(
        step,
        mesh=mesh,
        in_specs=(tokens, P(None), whole, whole, whole, whole),
        out_specs=tokens,
        check_vma=False,
    )
```

```python
import functools
import math

import jax
import jax.numpy as jnp
from jax import lax
from jax.experimental import pallas as pl
from jax.experimental.pallas import tpu as pltpu
from jax.sharding import PartitionSpec as P

HEAD = 256
THETA = 10000
NEG = -1e30
HIDDEN = 2 * NEG
LOG2E = 1.4426950408889634
MESH = pl.DeviceIdType.MESH
SLOTS = 3
RING = 14
TWO = 2
WIDTH = 512


def _dot(a, b, ca=1, cb=0):
    return lax.dot_general(a, b, (((ca,), (cb,)), ((), ())), preferred_element_type=jnp.float32)


def _offsets(side):
    far = lambda d: min(d, side - d)
    offsets = [(a, b) for a in range(side) for b in range(side)]
    offsets.sort(key=lambda o: (far(o[0]) + far(o[1]), max(far(o[0]), far(o[1])), min(o[0], o[1]) > 0 and o[0] != o[1], o[0] == 0))
    return offsets[1:] + offsets[:1]


def _pick(t, values):
    out = jnp.int32(values[-1])
    for i, v in enumerate(values[:-1]):
        out = jnp.where(t == i, jnp.int32(v), out)
    return out


def _flip(u, t):
    return lax.rem(u + t, 2) + 2 * lax.rem(u // 2 + t // 2, 2)


def _class(side, device):
    a, b = device // side % 2, device % side % 2
    return (2 - b) % 4 if a else 3 * b


def _kernel(n, x_ref, gain_ref, cos_ref, sin_ref, wq_ref, wk_ref, wv_ref, wo_ref, y_ref, x_s, a_s, w_s, out_s, q_s, k_s, v_s, wo_s, back_s, seen_s, acc_s,
            top_s, mix_s, x_sem, w_sem, wo_sem, send_sem, recv_sem, own_sem, back_send, back_recv, back_own, y_sem):
    side = math.isqrt(n)
    me = lax.axis_index("sp")
    high, low = me // side, lax.rem(me, side)
    own = x_s.shape[0]
    blocks = n // TWO
    offsets = _offsets(side)

    def to(t):
        a, b = _pick(t, [o[0] for o in offsets]), _pick(t, [o[1] for o in offsets])
        return lax.rem(high + a, side) * side + lax.rem(low + b, side)

    def frm(t):
        a, b = _pick(t, [o[0] for o in offsets]), _pick(t, [o[1] for o in offsets])
        return lax.rem(high - a + side, side) * side + lax.rem(low - b + side, side)

    classes = [_class(side, d) for d in range(n)]
    members = [[d for d in range(n) if classes[d] == u] for u in range(side)]
    my_class = _pick(me, classes)
    my_place = _pick(me, [members[classes[d]].index(d) for d in range(n)])
    own_pair = jnp.minimum(me // TWO, blocks - 1 - me // TWO)

    def head_at(r, a):
        return _pick(_flip(own_pair, r) * side + a, [d for some in members for d in some])

    def attends(i):
        return head_at(i // side, lax.rem(high + _pick(lax.rem(i, side), [1, 3, 2, 0]), side))

    serves = (to, to, attends)
    work = ((wv_ref, v_s), (wk_ref, k_s), (wq_ref, q_s))

    barrier = pltpu.get_barrier_semaphore()

    def greet(i, _):
        pl.semaphore_signal(barrier, inc=1, device_id={"sp": lax.rem(me + i, n)}, device_id_type=MESH)

    lax.fori_loop(1, n, greet, None)

    def fetch(m, t):
        slot = lax.rem(m * n + t, SLOTS)
        columns = pl.ds(pl.multiple_of(serves[m](t) * HEAD, HEAD), HEAD)
        return pltpu.make_async_copy(work[m][0].at[:, columns], w_s.at[slot], w_sem.at[slot])

    get_x = pltpu.make_async_copy(x_ref, x_s, x_sem)
    get_x.start()
    for t in range(SLOTS - 1):
        fetch(0, t).start()
    get_x.wait()

    rows = 32

    def norm(i, _):
        here = pl.ds(pl.multiple_of(i * rows, rows), rows)
        wide = x_s[here, :].astype(jnp.float32)
        scale = lax.rsqrt(jnp.mean(wide * wide, -1, keepdims=True) + 1e-6)
        a_s[here, :] = (wide * scale * gain_ref[...].astype(jnp.float32).reshape(1, -1)).astype(jnp.bfloat16)

    lax.fori_loop(0, own // rows, norm, None)
    pl.semaphore_wait(barrier, n - 1)

    def send(m, t, place, device):
        slot = lax.rem(m * n + t, RING)
        return pltpu.make_async_remote_copy(out_s.at[slot], work[m][1].at[place], send_sem.at[slot], recv_sem.at[m * n + place],
                                            device_id={"sp": device}, device_id_type=MESH)

    def keep(m, t):
        return pltpu.make_async_copy(out_s.at[lax.rem(m * n + t, RING)], work[m][1].at[me], own_sem)

    def pass_on(m, t):
        device = serves[m](t)

        @pl.when(device != me)
        def _():
            send(m, t, me, device).start()

        @pl.when(device == me)
        def _():
            keep(m, t).start()
            keep(m, t).wait()

    def passed(m, t):
        device = serves[m](t)

        @pl.when(device != me)
        def _():
            send(m, t, me, device).wait_send()

    for m in range(3):

        def step(t, _, m=m):
            ahead = t + SLOTS - 1

            @pl.when(ahead < n)
            def _():
                fetch(m, ahead).start()

            if m < 2:
                @pl.when(ahead >= n)
                def _():
                    fetch(m + 1, ahead - n).start()

            @pl.when(t > 0)
            def _():
                pass_on(m, t - 1)

            @pl.when(t >= RING)
            def _():
                passed(m, t - RING)

            if m > 0:
                @pl.when(t < RING)
                def _():
                    passed(m - 1, t + n - RING)

            fetch(m, t).wait()
            made = _dot(a_s[...], w_s[lax.rem(m * n + t, SLOTS)]).astype(jnp.bfloat16).astype(jnp.float32)
            if m != 0:
                a, b = made[:, : HEAD // 2], made[:, HEAD // 2 :]
                cos, sin = cos_ref[...], sin_ref[...]
                made = jnp.concatenate([a * cos - b * sin, b * cos + a * sin], axis=1)
            if m != 1:
                made = made.T
            out_s[lax.rem(m * n + t, RING)] = made.astype(jnp.bfloat16)

        lax.fori_loop(0, n, step, None)
        pass_on(m, n - 1)

    def fetch_out(i):
        return pltpu.make_async_copy(wo_ref.at[pl.ds(pl.multiple_of(head_at(i // side, lax.rem(i, side)) * HEAD, HEAD), HEAD), :], wo_s.at[i], wo_sem.at[i])

    lax.fori_loop(0, n, lambda i, _: fetch_out(i).start(), None)
    acc_s[...] = x_s[...].astype(jnp.float32)

    for m in range(2):

        def came(t, _, m=m):
            send(m, t, frm(t), to(t)).wait_recv()

        lax.fori_loop(0, n - 1, came, None)

    e = HEAD**-0.5 * LOG2E
    size = TWO * own

    def block(p, j, many, masked):
        keys = [k_s[pl.ds((j + c) * TWO, TWO)].reshape(size, HEAD) for c in range(many)]
        values = jnp.concatenate([v_s[j * TWO + c] for c in range(TWO * many)], axis=1)
        values = jnp.concatenate([values, jnp.ones((8, size * many), jnp.bfloat16)], axis=0)
        scores = [[_dot(some, q_s[p * TWO + i]) for some in keys] for i in range(TWO)]
        weights, keeps = [], []
        for i, parts in enumerate(scores):
            if masked:
                gap = lax.broadcasted_iota(jnp.int32, (size, own), 1) - lax.broadcasted_iota(jnp.int32, (size, own), 0)
                parts[-1] = jnp.where(gap >= -i * own, parts[-1], HIDDEN)
            old = top_s[i : i + 1, :]
            top = old
            for s in parts:
                top = jnp.maximum(top, s.max(axis=0, keepdims=True))
            top_s[i : i + 1, :] = top
            weights.append(jnp.concatenate([jnp.exp2((s - top) * e).astype(jnp.bfloat16) for s in parts], axis=0))
            keeps.append(jnp.exp2((old - top) * e))
        for i in range(TWO):
            mix_s[i] = mix_s[i] * keeps[i] + _dot(values, weights[i])

    def seen(r, a):
        return seen_s.at[r, :, pl.ds(pl.multiple_of(a * HEAD, HEAD), HEAD)]

    def back(dest, r, a):
        return pltpu.make_async_remote_copy(back_s.at[dest], seen(r, a), back_send.at[dest], back_recv.at[r * side + a], device_id={"sp": dest},
                                            device_id_type=MESH)

    def back_keep(r):
        return pltpu.make_async_copy(back_s.at[me], seen(r, my_place), back_own)

    def attend(i, _):
        r = i // 2
        u = _flip(my_class, r)
        p = jnp.where(lax.rem(i, 2) == 0, u, blocks - 1 - u)
        for c in range(TWO):
            source = p * TWO + c

            @pl.when(source != me)
            def _():
                send(2, 0, source, source).wait_recv()

        top_s[...] = jnp.full_like(top_s, NEG)
        mix_s[...] = jnp.zeros_like(mix_s)
        lax.fori_loop(0, p // 2, lambda j, _: block(p, 2 * j, 2, False), None)

        @pl.when(lax.rem(p, 2) == 1)
        def _():
            block(p, p - 1, 2, True)

        @pl.when(lax.rem(p, 2) == 0)
        def _():
            block(p, p, 1, True)

        for c in range(TWO):
            total = mix_s[c, HEAD : HEAD + 1, :]
            back_s[p * TWO + c] = (mix_s[c, :HEAD, :] * (1 / total)).T.astype(jnp.bfloat16)
        for c in range(TWO):
            dest = p * TWO + c

            @pl.when(dest != me)
            def _():
                back(dest, r, my_place).start()

            @pl.when(dest == me)
            def _():
                back_keep(r).start()

    lax.fori_loop(0, blocks, attend, None)

    def arrive(r):
        for a in range(side):
            head = head_at(r, a)

            @pl.when(head != me)
            def _():
                back(head, r, a).wait_recv()

            @pl.when(head == me)
            def _():
                back_keep(r).wait()

            fetch_out(r * side + a).wait()

    def weights_of(r, here):
        return wo_s[pl.ds(r * side, side), :, here].reshape(side * HEAD, WIDTH)

    def columns(c):
        return pl.ds(pl.multiple_of(c * WIDTH, WIDTH), WIDTH)

    def gather(r, _):
        arrive(r)

        def part(c, _):
            here = columns(c)
            acc_s[:, here] += _dot(seen_s[r], weights_of(r, here))

        lax.fori_loop(0, acc_s.shape[1] // WIDTH, part, None)

    lax.fori_loop(0, side - 1, gather, None)
    arrive(side - 1)

    def put(c):
        return pltpu.make_async_copy(x_s.at[:, columns(c)], y_ref.at[:, columns(c)], y_sem.at[c])

    def last(c, _):
        here = columns(c)
        x_s[:, here] = (acc_s[:, here] + _dot(seen_s[side - 1], weights_of(side - 1, here))).astype(jnp.bfloat16)
        put(c).start()

    chunks = acc_s.shape[1] // WIDTH
    lax.fori_loop(0, chunks, last, None)
    lax.fori_loop(n - RING, n, lambda t, _: passed(2, t), None)

    def gone(i, _):
        dest = lax.rem(me + i, n)
        back(dest, 0, 0).wait_send()

    lax.fori_loop(1, n, gone, None)
    lax.fori_loop(0, chunks, lambda c, _: put(c).wait(), None)


def solution(mesh):
    n = mesh.shape["sp"]
    side = math.isqrt(n)
    any_, vmem = pl.BlockSpec(memory_space=pl.ANY), pl.BlockSpec(memory_space=pltpu.VMEM)
    low, wide = jnp.bfloat16, jnp.float32

    def step(x, gain, wq, wk, wv, wo):
        own, d = x.shape
        half = HEAD // 2
        place = (lax.axis_index("sp") * own + jnp.arange(own)).astype(wide)
        angle = place[:, None] * THETA ** (-jnp.arange(half, dtype=wide) / half)
        dma = lambda *shape: pltpu.SemaphoreType.DMA(shape)
        return pl.pallas_call(
            functools.partial(_kernel, n),
            out_shape=jax.ShapeDtypeStruct((own, d), low),
            in_specs=[any_] + [vmem] * 3 + [any_] * 4,
            out_specs=any_,
            scratch_shapes=[
                pltpu.VMEM((own, d), low),
                pltpu.VMEM((own, d), low),
                pltpu.VMEM((SLOTS, d, HEAD), low),
                pltpu.VMEM((RING, own, HEAD), low),
                pltpu.VMEM((n, HEAD, own), low),
                pltpu.VMEM((n, own, HEAD), low),
                pltpu.VMEM((n, HEAD, own), low),
                pltpu.VMEM((n, HEAD, d), low),
                pltpu.VMEM((n, own, HEAD), low),
                pltpu.VMEM((side, own, side * HEAD), low),
                pltpu.VMEM((own, d), wide),
                pltpu.VMEM((TWO, own), wide),
                pltpu.VMEM((TWO, HEAD + 8, own), wide),
                dma(), dma(SLOTS), dma(n), dma(RING), dma(3 * n), dma(), dma(n), dma(n), dma(), dma(d // WIDTH),
            ],
            compiler_params=pltpu.CompilerParams(collective_id=0, has_side_effects=True, vmem_limit_bytes=61 * 2**20),
            cost_estimate=pl.CostEstimate(flops=10 * own * d * d, transcendentals=0, bytes_accessed=8 * d * d),
        )(x, gain, jnp.cos(angle), jnp.sin(angle), wq, wk, wv, wo)

    tokens, whole = P(("dp", "sp"), None), P(None, None)
    return jax.shard_map(
        step,
        mesh=mesh,
        in_specs=(tokens, P(None), whole, whole, whole, whole),
        out_specs=tokens,
        check_vma=False,
    )
```

```python
import functools
import math

import jax
import jax.numpy as jnp
from jax import lax
from jax.experimental import pallas as pl
from jax.experimental.pallas import tpu as pltpu
from jax.sharding import PartitionSpec as P

HEAD = 256
THETA = 10000
NEG = -1e30
HIDDEN = 2 * NEG
LOG2E = 1.4426950408889634
MESH = pl.DeviceIdType.MESH
SLOTS = 3
RING = 14
TWO = 2
WIDTH = 512


def _dot(a, b, ca=1, cb=0):
    return lax.dot_general(a, b, (((ca,), (cb,)), ((), ())), preferred_element_type=jnp.float32)


def _offsets(side):
    far = lambda d: min(d, side - d)
    offsets = [(a, b) for a in range(side) for b in range(side)]
    offsets.sort(key=lambda o: (far(o[0]) + far(o[1]), max(far(o[0]), far(o[1])), min(o[0], o[1]) > 0 and o[0] != o[1], o[0] == 0))
    return offsets[1:] + offsets[:1]


def _pick(t, values):
    out = jnp.int32(values[-1])
    for i, v in enumerate(values[:-1]):
        out = jnp.where(t == i, jnp.int32(v), out)
    return out


def _flip(u, t):
    return lax.rem(u + t, 2) + 2 * lax.rem(u // 2 + t // 2, 2)


def _class(side, device):
    a, b = device // side % 2, device % side % 2
    return (2 - b) % 4 if a else 3 * b


def _kernel(n, x_ref, gain_ref, turn_ref, wq_ref, wk_ref, wv_ref, wo_ref, y_ref, x_s, gain_s, turn_s, a_s, w_s, out_s, q_s, k_s, v_s, wo_s, back_s, seen_s, acc_s,
            top_s, mix_s, x_sem, turn_sem, w_sem, wo_sem, send_sem, recv_sem, own_sem, back_send, back_recv, back_own, y_sem):
    side = math.isqrt(n)
    me = lax.axis_index("sp")
    high, low = me // side, lax.rem(me, side)
    own = x_s.shape[0]
    blocks = n // TWO
    offsets = _offsets(side)

    def to(t):
        a, b = _pick(t, [o[0] for o in offsets]), _pick(t, [o[1] for o in offsets])
        return lax.rem(high + a, side) * side + lax.rem(low + b, side)

    def frm(t):
        a, b = _pick(t, [o[0] for o in offsets]), _pick(t, [o[1] for o in offsets])
        return lax.rem(high - a + side, side) * side + lax.rem(low - b + side, side)

    classes = [_class(side, d) for d in range(n)]
    members = [[d for d in range(n) if classes[d] == u] for u in range(side)]
    my_class = _pick(me, classes)
    my_place = _pick(me, [members[classes[d]].index(d) for d in range(n)])
    own_pair = jnp.minimum(me // TWO, blocks - 1 - me // TWO)

    def head_at(r, a):
        return _pick(_flip(own_pair, r) * side + a, [d for some in members for d in some])

    def attends(i):
        return head_at(i // side, lax.rem(high + _pick(lax.rem(i, side), [1, 3, 2, 0]), side))

    serves = (to, to, attends)
    work = ((wv_ref, v_s), (wk_ref, k_s), (wq_ref, q_s))

    barrier = pltpu.get_barrier_semaphore()

    def greet(i, _):
        pl.semaphore_signal(barrier, inc=1, device_id={"sp": lax.rem(me + i, n)}, device_id_type=MESH)

    lax.fori_loop(1, n, greet, None)

    def fetch(m, t):
        slot = lax.rem(m * n + t, SLOTS)
        columns = pl.ds(pl.multiple_of(serves[m](t) * HEAD, HEAD), HEAD)
        return pltpu.make_async_copy(work[m][0].at[:, columns], w_s.at[slot], w_sem.at[slot])

    get_x = pltpu.make_async_copy(x_ref, x_s, x_sem)
    get_x.start()
    get_turn = pltpu.make_async_copy(turn_ref, turn_s, turn_sem)
    for t in range(SLOTS - 1):
        fetch(0, t).start()
    get_turn.start()
    gain_s[...] = gain_ref[...].astype(jnp.float32).reshape(1, -1)
    get_x.wait()

    rows = 32

    def norm(i, _):
        here = pl.ds(pl.multiple_of(i * rows, rows), rows)
        wide = x_s[here, :].astype(jnp.float32)
        scale = lax.rsqrt(jnp.mean(wide * wide, -1, keepdims=True) + 1e-6)
        a_s[here, :] = (wide * scale * gain_s[...]).astype(jnp.bfloat16)

    lax.fori_loop(0, own // rows, norm, None)
    pl.semaphore_wait(barrier, n - 1)

    def send(m, t, place, device):
        slot = lax.rem(m * n + t, RING)
        return pltpu.make_async_remote_copy(out_s.at[slot], work[m][1].at[place], send_sem.at[slot], recv_sem.at[m * n + place],
                                            device_id={"sp": device}, device_id_type=MESH)

    def keep(m, t):
        return pltpu.make_async_copy(out_s.at[lax.rem(m * n + t, RING)], work[m][1].at[me], own_sem)

    def pass_on(m, t):
        device = serves[m](t)

        @pl.when(device != me)
        def _():
            send(m, t, me, device).start()

        @pl.when(device == me)
        def _():
            keep(m, t).start()
            keep(m, t).wait()

    def passed(m, t):
        device = serves[m](t)

        @pl.when(device != me)
        def _():
            send(m, t, me, device).wait_send()

    for m in range(3):
        if m == 1:
            get_turn.wait()

        def step(t, _, m=m):
            ahead = t + SLOTS - 1

            @pl.when(ahead < n)
            def _():
                fetch(m, ahead).start()

            if m < 2:
                @pl.when(ahead >= n)
                def _():
                    fetch(m + 1, ahead - n).start()

            @pl.when(t > 0)
            def _():
                pass_on(m, t - 1)

            @pl.when(t >= RING)
            def _():
                passed(m, t - RING)

            if m > 0:
                @pl.when(t < RING)
                def _():
                    passed(m - 1, t + n - RING)

            fetch(m, t).wait()
            made = _dot(a_s[...], w_s[lax.rem(m * n + t, SLOTS)]).astype(jnp.bfloat16).astype(jnp.float32)
            if m != 0:
                a, b = made[:, : HEAD // 2], made[:, HEAD // 2 :]
                cos, sin = turn_s[0], turn_s[1]
                made = jnp.concatenate([a * cos - b * sin, b * cos + a * sin], axis=1)
            if m != 1:
                made = made.T
            out_s[lax.rem(m * n + t, RING)] = made.astype(jnp.bfloat16)

        lax.fori_loop(0, n, step, None)
        pass_on(m, n - 1)

    def fetch_out(i):
        return pltpu.make_async_copy(wo_ref.at[pl.ds(pl.multiple_of(head_at(i // side, lax.rem(i, side)) * HEAD, HEAD), HEAD), :], wo_s.at[i], wo_sem.at[i])

    lax.fori_loop(0, n, lambda i, _: fetch_out(i).start(), None)
    acc_s[...] = x_s[...].astype(jnp.float32)

    for m in range(2):

        def came(t, _, m=m):
            send(m, t, frm(t), to(t)).wait_recv()

        lax.fori_loop(0, n - 1, came, None)

    e = HEAD**-0.5 * LOG2E
    size = TWO * own

    def block(p, j, many, masked):
        keys = [k_s[pl.ds((j + c) * TWO, TWO)].reshape(size, HEAD) for c in range(many)]
        values = jnp.concatenate([v_s[j * TWO + c] for c in range(TWO * many)], axis=1)
        values = jnp.concatenate([values, jnp.ones((8, size * many), jnp.bfloat16)], axis=0)
        scores = [[_dot(some, q_s[p * TWO + i]) for some in keys] for i in range(TWO)]
        weights, keeps = [], []
        for i, parts in enumerate(scores):
            if masked:
                gap = lax.broadcasted_iota(jnp.int32, (size, own), 1) - lax.broadcasted_iota(jnp.int32, (size, own), 0)
                parts[-1] = jnp.where(gap >= -i * own, parts[-1], HIDDEN)
            old = top_s[i : i + 1, :]
            top = old
            for s in parts:
                top = jnp.maximum(top, s.max(axis=0, keepdims=True))
            top_s[i : i + 1, :] = top
            weights.append(jnp.concatenate([jnp.exp2((s - top) * e).astype(jnp.bfloat16) for s in parts], axis=0))
            keeps.append(jnp.exp2((old - top) * e))
        for i in range(TWO):
            mix_s[i] = mix_s[i] * keeps[i] + _dot(values, weights[i])

    def seen(r, a):
        return seen_s.at[r, a]

    def back(dest, r, a):
        return pltpu.make_async_remote_copy(back_s.at[dest], seen(r, a), back_send.at[dest], back_recv.at[r * side + a], device_id={"sp": dest},
                                            device_id_type=MESH)

    def back_keep(r):
        return pltpu.make_async_copy(back_s.at[me], seen(r, my_place), back_own)

    def attend(i, _):
        r = i // 2
        u = _flip(my_class, r)
        p = jnp.where(lax.rem(i, 2) == 0, u, blocks - 1 - u)
        for c in range(TWO):
            source = p * TWO + c

            @pl.when(source != me)
            def _():
                send(2, 0, source, source).wait_recv()

        top_s[...] = jnp.full_like(top_s, NEG)
        mix_s[...] = jnp.zeros_like(mix_s)
        lax.fori_loop(0, p // 2, lambda j, _: block(p, 2 * j, 2, False), None)

        @pl.when(lax.rem(p, 2) == 1)
        def _():
            block(p, p - 1, 2, True)

        @pl.when(lax.rem(p, 2) == 0)
        def _():
            block(p, p, 1, True)

        for c in range(TWO):
            total = mix_s[c, HEAD : HEAD + 1, :]
            back_s[p * TWO + c] = (mix_s[c, :HEAD, :] * (1 / total)).T.astype(jnp.bfloat16)
        for c in range(TWO):
            dest = p * TWO + c

            @pl.when(dest != me)
            def _():
                back(dest, r, my_place).start()

            @pl.when(dest == me)
            def _():
                back_keep(r).start()

    lax.fori_loop(0, blocks, attend, None)

    def arrive(r):
        for a in range(side):
            head = head_at(r, a)

            @pl.when(head != me)
            def _():
                back(head, r, a).wait_recv()

            @pl.when(head == me)
            def _():
                back_keep(r).wait()

            fetch_out(r * side + a).wait()

    def seen_of(r):
        return jnp.concatenate([seen_s[r, a] for a in range(side)], axis=1)

    def weights_of(r, here):
        return wo_s[pl.ds(r * side, side), :, here].reshape(side * HEAD, WIDTH)

    def columns(c):
        return pl.ds(pl.multiple_of(c * WIDTH, WIDTH), WIDTH)

    def gather(r, _):
        arrive(r)

        def part(c, _):
            here = columns(c)
            acc_s[:, here] += _dot(seen_of(r), weights_of(r, here))

        lax.fori_loop(0, acc_s.shape[1] // WIDTH, part, None)

    lax.fori_loop(0, side - 1, gather, None)
    arrive(side - 1)

    def put(c):
        return pltpu.make_async_copy(x_s.at[:, columns(c)], y_ref.at[:, columns(c)], y_sem.at[c])

    def last(c, _):
        here = columns(c)
        x_s[:, here] = (acc_s[:, here] + _dot(seen_of(side - 1), weights_of(side - 1, here))).astype(jnp.bfloat16)
        put(c).start()

    chunks = acc_s.shape[1] // WIDTH
    lax.fori_loop(0, chunks, last, None)
    lax.fori_loop(n - RING, n, lambda t, _: passed(2, t), None)

    def gone(i, _):
        dest = lax.rem(me + i, n)
        back(dest, 0, 0).wait_send()

    lax.fori_loop(1, n, gone, None)
    lax.fori_loop(0, chunks, lambda c, _: put(c).wait(), None)


def solution(mesh):
    n = mesh.shape["sp"]
    side = math.isqrt(n)
    any_, vmem = pl.BlockSpec(memory_space=pl.ANY), pl.BlockSpec(memory_space=pltpu.VMEM)
    low, wide = jnp.bfloat16, jnp.float32

    def step(x, gain, wq, wk, wv, wo):
        own, d = x.shape
        half = HEAD // 2
        place = (lax.axis_index("sp") * own + jnp.arange(own)).astype(wide)
        angle = place[:, None] * THETA ** (-jnp.arange(half, dtype=wide) / half)
        dma = lambda *shape: pltpu.SemaphoreType.DMA(shape)
        return pl.pallas_call(
            functools.partial(_kernel, n),
            out_shape=jax.ShapeDtypeStruct((own, d), low),
            in_specs=[any_, vmem] + [any_] * 5,
            out_specs=any_,
            scratch_shapes=[
                pltpu.VMEM((own, d), low),
                pltpu.VMEM((1, d), wide),
                pltpu.VMEM((2, own, half), wide),
                pltpu.VMEM((own, d), low),
                pltpu.VMEM((SLOTS, d, HEAD), low),
                pltpu.VMEM((RING, own, HEAD), low),
                pltpu.VMEM((n, HEAD, own), low),
                pltpu.VMEM((n, own, HEAD), low),
                pltpu.VMEM((n, HEAD, own), low),
                pltpu.VMEM((n, HEAD, d), low),
                pltpu.VMEM((n, own, HEAD), low),
                pltpu.VMEM((side, side, own, HEAD), low),
                pltpu.VMEM((own, d), wide),
                pltpu.VMEM((TWO, own), wide),
                pltpu.VMEM((TWO, HEAD + 8, own), wide),
                dma(), dma(), dma(SLOTS), dma(n), dma(RING), dma(3 * n), dma(), dma(n), dma(n), dma(), dma(d // WIDTH),
            ],
            compiler_params=pltpu.CompilerParams(collective_id=0, has_side_effects=True, vmem_limit_bytes=61 * 2**20),
            cost_estimate=pl.CostEstimate(flops=10 * own * d * d, transcendentals=0, bytes_accessed=8 * d * d),
        )(x, gain, jnp.stack([jnp.cos(angle), jnp.sin(angle)]), wq, wk, wv, wo)

    tokens, whole = P(("dp", "sp"), None), P(None, None)
    return jax.shard_map(
        step,
        mesh=mesh,
        in_specs=(tokens, P(None), whole, whole, whole, whole),
        out_specs=tokens,
        check_vma=False,
    )
```

```python
import functools
import math

import jax
import jax.numpy as jnp
from jax import lax
from jax.experimental import pallas as pl
from jax.experimental.pallas import tpu as pltpu
from jax.sharding import PartitionSpec as P

HEAD = 256
THETA = 10000
NEG = -1e30
HIDDEN = 2 * NEG
LOG2E = 1.4426950408889634
MESH = pl.DeviceIdType.MESH
SLOTS = 3
RING = 14
TWO = 2
WIDTH = 1024


def _dot(a, b, ca=1, cb=0):
    return lax.dot_general(a, b, (((ca,), (cb,)), ((), ())), preferred_element_type=jnp.float32)


def _offsets(side):
    far = lambda d: min(d, side - d)
    offsets = [(a, b) for a in range(side) for b in range(side)]
    offsets.sort(key=lambda o: (far(o[0]) + far(o[1]), max(far(o[0]), far(o[1])), min(o[0], o[1]) > 0 and o[0] != o[1], o[0] == 0))
    return offsets[1:] + offsets[:1]


def _pick(t, values):
    out = jnp.int32(values[-1])
    for i, v in enumerate(values[:-1]):
        out = jnp.where(t == i, jnp.int32(v), out)
    return out


def _flip(u, t):
    return lax.rem(u + t, 2) + 2 * lax.rem(u // 2 + t // 2, 2)


def _class(side, device):
    a, b = device // side % 2, device % side % 2
    return (2 - b) % 4 if a else 3 * b


def _kernel(n, x_ref, gain_ref, turn_ref, wq_ref, wk_ref, wv_ref, wo_ref, y_ref, x_s, gain_s, turn_s, a_s, w_s, out_s, q_s, k_s, v_s, wo_s, back_s, seen_s, acc_s,
            top_s, mix_s, x_sem, turn_sem, w_sem, wo_sem, send_sem, recv_sem, own_sem, back_send, back_recv, back_own, y_sem):
    side = math.isqrt(n)
    me = lax.axis_index("sp")
    high, low = me // side, lax.rem(me, side)
    own = x_s.shape[0]
    blocks = n // TWO
    offsets = _offsets(side)

    def to(t):
        a, b = _pick(t, [o[0] for o in offsets]), _pick(t, [o[1] for o in offsets])
        return lax.rem(high + a, side) * side + lax.rem(low + b, side)

    def frm(t):
        a, b = _pick(t, [o[0] for o in offsets]), _pick(t, [o[1] for o in offsets])
        return lax.rem(high - a + side, side) * side + lax.rem(low - b + side, side)

    classes = [_class(side, d) for d in range(n)]
    members = [[d for d in range(n) if classes[d] == u] for u in range(side)]
    my_class = _pick(me, classes)
    my_place = _pick(me, [members[classes[d]].index(d) for d in range(n)])
    own_pair = jnp.minimum(me // TWO, blocks - 1 - me // TWO)

    def head_at(r, a):
        return _pick(_flip(own_pair, r) * side + a, [d for some in members for d in some])

    def attends(i):
        return head_at(i // side, lax.rem(high + _pick(lax.rem(i, side), [1, 3, 2, 0]), side))

    serves = (to, to, attends)
    work = ((wv_ref, v_s), (wk_ref, k_s), (wq_ref, q_s))

    barrier = pltpu.get_barrier_semaphore()

    def greet(i, _):
        pl.semaphore_signal(barrier, inc=1, device_id={"sp": lax.rem(me + i, n)}, device_id_type=MESH)

    lax.fori_loop(1, n, greet, None)

    def fetch(m, t):
        slot = lax.rem(m * n + t, SLOTS)
        columns = pl.ds(pl.multiple_of(serves[m](t) * HEAD, HEAD), HEAD)
        return pltpu.make_async_copy(work[m][0].at[:, columns], w_s.at[slot], w_sem.at[slot])

    get_x = pltpu.make_async_copy(x_ref, x_s, x_sem)
    get_x.start()
    get_turn = pltpu.make_async_copy(turn_ref, turn_s, turn_sem)
    for t in range(SLOTS - 1):
        fetch(0, t).start()
    get_turn.start()
    gain_s[...] = gain_ref[...].astype(jnp.float32).reshape(1, -1)
    get_x.wait()

    rows = 32

    def norm(i, _):
        here = pl.ds(pl.multiple_of(i * rows, rows), rows)
        wide = x_s[here, :].astype(jnp.float32)
        scale = lax.rsqrt(jnp.mean(wide * wide, -1, keepdims=True) + 1e-6)
        a_s[here, :] = (wide * scale * gain_s[...]).astype(jnp.bfloat16)

    lax.fori_loop(0, own // rows, norm, None)
    pl.semaphore_wait(barrier, n - 1)

    def send(m, t, place, device):
        slot = lax.rem(m * n + t, RING)
        return pltpu.make_async_remote_copy(out_s.at[slot], work[m][1].at[place], send_sem.at[slot], recv_sem.at[m * n + place],
                                            device_id={"sp": device}, device_id_type=MESH)

    def keep(m, t):
        return pltpu.make_async_copy(out_s.at[lax.rem(m * n + t, RING)], work[m][1].at[me], own_sem)

    def pass_on(m, t):
        device = serves[m](t)

        @pl.when(device != me)
        def _():
            send(m, t, me, device).start()

        @pl.when(device == me)
        def _():
            keep(m, t).start()
            keep(m, t).wait()

    def passed(m, t):
        device = serves[m](t)

        @pl.when(device != me)
        def _():
            send(m, t, me, device).wait_send()

    for m in range(3):
        if m == 1:
            get_turn.wait()

        def step(t, _, m=m):
            ahead = t + SLOTS - 1

            @pl.when(ahead < n)
            def _():
                fetch(m, ahead).start()

            if m < 2:
                @pl.when(ahead >= n)
                def _():
                    fetch(m + 1, ahead - n).start()

            @pl.when(t > 0)
            def _():
                pass_on(m, t - 1)

            @pl.when(t >= RING)
            def _():
                passed(m, t - RING)

            if m > 0:
                @pl.when(t < RING)
                def _():
                    passed(m - 1, t + n - RING)

            fetch(m, t).wait()
            made = _dot(a_s[...], w_s[lax.rem(m * n + t, SLOTS)]).astype(jnp.bfloat16).astype(jnp.float32)
            if m != 0:
                a, b = made[:, : HEAD // 2], made[:, HEAD // 2 :]
                cos, sin = turn_s[0], turn_s[1]
                made = jnp.concatenate([a * cos - b * sin, b * cos + a * sin], axis=1)
            if m != 1:
                made = made.T
            out_s[lax.rem(m * n + t, RING)] = made.astype(jnp.bfloat16)

        lax.fori_loop(0, n, step, None)
        pass_on(m, n - 1)

    def fetch_out(i):
        return pltpu.make_async_copy(wo_ref.at[pl.ds(pl.multiple_of(head_at(i // side, lax.rem(i, side)) * HEAD, HEAD), HEAD), :], wo_s.at[i], wo_sem.at[i])

    lax.fori_loop(0, n, lambda i, _: fetch_out(i).start(), None)
    acc_s[...] = x_s[...].astype(jnp.float32)

    for m in range(2):

        def came(t, _, m=m):
            send(m, t, frm(t), to(t)).wait_recv()

        lax.fori_loop(0, n - 1, came, None)

    e = HEAD**-0.5 * LOG2E
    size = TWO * own

    def block(p, j, many, masked):
        keys = [k_s[pl.ds((j + c) * TWO, TWO)].reshape(size, HEAD) for c in range(many)]
        values = jnp.concatenate([v_s[j * TWO + c] for c in range(TWO * many)], axis=1)
        values = jnp.concatenate([values, jnp.ones((8, size * many), jnp.bfloat16)], axis=0)
        scores = [[_dot(some, q_s[p * TWO + i]) for some in keys] for i in range(TWO)]
        weights, keeps = [], []
        for i, parts in enumerate(scores):
            if masked:
                gap = lax.broadcasted_iota(jnp.int32, (size, own), 1) - lax.broadcasted_iota(jnp.int32, (size, own), 0)
                parts[-1] = jnp.where(gap >= -i * own, parts[-1], HIDDEN)
            old = top_s[i : i + 1, :]
            top = old
            for s in parts:
                top = jnp.maximum(top, s.max(axis=0, keepdims=True))
            top_s[i : i + 1, :] = top
            weights.append(jnp.concatenate([jnp.exp2((s - top) * e).astype(jnp.bfloat16) for s in parts], axis=0))
            keeps.append(jnp.exp2((old - top) * e))
        for i in range(TWO):
            mix_s[i] = mix_s[i] * keeps[i] + _dot(values, weights[i])

    def seen(r, a):
        return seen_s.at[r, a]

    def back(dest, r, a):
        return pltpu.make_async_remote_copy(back_s.at[dest], seen(r, a), back_send.at[dest], back_recv.at[r * side + a], device_id={"sp": dest},
                                            device_id_type=MESH)

    def back_keep(r):
        return pltpu.make_async_copy(back_s.at[me], seen(r, my_place), back_own)

    def attend(i, _):
        r = i // 2
        u = _flip(my_class, r)
        p = jnp.where(lax.rem(i, 2) == 0, u, blocks - 1 - u)
        for c in range(TWO):
            source = p * TWO + c

            @pl.when(source != me)
            def _():
                send(2, 0, source, source).wait_recv()

        top_s[...] = jnp.full_like(top_s, NEG)
        mix_s[...] = jnp.zeros_like(mix_s)
        lax.fori_loop(0, p // 2, lambda j, _: block(p, 2 * j, 2, False), None)

        @pl.when(lax.rem(p, 2) == 1)
        def _():
            block(p, p - 1, 2, True)

        @pl.when(lax.rem(p, 2) == 0)
        def _():
            block(p, p, 1, True)

        for c in range(TWO):
            total = mix_s[c, HEAD : HEAD + 1, :]
            back_s[p * TWO + c] = (mix_s[c, :HEAD, :] * (1 / total)).T.astype(jnp.bfloat16)
        for c in range(TWO):
            dest = p * TWO + c

            @pl.when(dest != me)
            def _():
                back(dest, r, my_place).start()

            @pl.when(dest == me)
            def _():
                back_keep(r).start()

    lax.fori_loop(0, blocks, attend, None)

    def arrive(r):
        for a in range(side):
            head = head_at(r, a)

            @pl.when(head != me)
            def _():
                back(head, r, a).wait_recv()

            @pl.when(head == me)
            def _():
                back_keep(r).wait()

            fetch_out(r * side + a).wait()

    def seen_of(r):
        return jnp.concatenate([seen_s[r, a] for a in range(side)], axis=1)

    def weights_of(r, here):
        return wo_s[pl.ds(r * side, side), :, here].reshape(side * HEAD, WIDTH)

    def columns(c):
        return pl.ds(pl.multiple_of(c * WIDTH, WIDTH), WIDTH)

    def gather(r, _):
        arrive(r)

        def part(c, _):
            here = columns(c)
            acc_s[:, here] += _dot(seen_of(r), weights_of(r, here))

        lax.fori_loop(0, acc_s.shape[1] // WIDTH, part, None)

    lax.fori_loop(0, side - 1, gather, None)
    arrive(side - 1)

    def put(c):
        return pltpu.make_async_copy(x_s.at[:, columns(c)], y_ref.at[:, columns(c)], y_sem.at[c])

    def last(c, _):
        here = columns(c)
        x_s[:, here] = (acc_s[:, here] + _dot(seen_of(side - 1), weights_of(side - 1, here))).astype(jnp.bfloat16)
        put(c).start()

    chunks = acc_s.shape[1] // WIDTH
    lax.fori_loop(0, chunks, last, None)
    lax.fori_loop(n - RING, n, lambda t, _: passed(2, t), None)

    def gone(i, _):
        dest = lax.rem(me + i, n)
        back(dest, 0, 0).wait_send()

    lax.fori_loop(1, n, gone, None)
    lax.fori_loop(0, chunks, lambda c, _: put(c).wait(), None)


def solution(mesh):
    n = mesh.shape["sp"]
    side = math.isqrt(n)
    any_, vmem = pl.BlockSpec(memory_space=pl.ANY), pl.BlockSpec(memory_space=pltpu.VMEM)
    low, wide = jnp.bfloat16, jnp.float32

    def step(x, gain, wq, wk, wv, wo):
        own, d = x.shape
        half = HEAD // 2
        place = (lax.axis_index("sp") * own + jnp.arange(own)).astype(wide)
        angle = place[:, None] * THETA ** (-jnp.arange(half, dtype=wide) / half)
        dma = lambda *shape: pltpu.SemaphoreType.DMA(shape)
        return pl.pallas_call(
            functools.partial(_kernel, n),
            out_shape=jax.ShapeDtypeStruct((own, d), low),
            in_specs=[any_, vmem] + [any_] * 5,
            out_specs=any_,
            scratch_shapes=[
                pltpu.VMEM((own, d), low),
                pltpu.VMEM((1, d), wide),
                pltpu.VMEM((2, own, half), wide),
                pltpu.VMEM((own, d), low),
                pltpu.VMEM((SLOTS, d, HEAD), low),
                pltpu.VMEM((RING, own, HEAD), low),
                pltpu.VMEM((n, HEAD, own), low),
                pltpu.VMEM((n, own, HEAD), low),
                pltpu.VMEM((n, HEAD, own), low),
                pltpu.VMEM((n, HEAD, d), low),
                pltpu.VMEM((n, own, HEAD), low),
                pltpu.VMEM((side, side, own, HEAD), low),
                pltpu.VMEM((own, d), wide),
                pltpu.VMEM((TWO, own), wide),
                pltpu.VMEM((TWO, HEAD + 8, own), wide),
                dma(), dma(), dma(SLOTS), dma(n), dma(RING), dma(3 * n), dma(), dma(n), dma(n), dma(), dma(d // WIDTH),
            ],
            compiler_params=pltpu.CompilerParams(collective_id=0, has_side_effects=True, vmem_limit_bytes=61 * 2**20),
            cost_estimate=pl.CostEstimate(flops=10 * own * d * d, transcendentals=0, bytes_accessed=8 * d * d),
        )(x, gain, jnp.stack([jnp.cos(angle), jnp.sin(angle)]), wq, wk, wv, wo)

    tokens, whole = P(("dp", "sp"), None), P(None, None)
    return jax.shard_map(
        step,
        mesh=mesh,
        in_specs=(tokens, P(None), whole, whole, whole, whole),
        out_specs=tokens,
        check_vma=False,
    )
```
